32 devices in a mesh: dp: 1, sp: 32 (over x, y, z, core).
Axes of the slice: x: 2, y: 2, z: 4, core: 2. Of those that a mesh axis runs over, the one named last changes fastest.
Arguments:
- q: bfloat16 [32, 64, 112], P('dp')
- k: bfloat16 [32, 4096, 64, 112], P('dp', 'sp')
- v: bfloat16 [32, 4096, 64, 112], P('dp', 'sp')
Outputs:
- q: bfloat16 [32, 64, 112], P('dp')
All inputs are finite; a program needn't handle non-finite values.
Results may differ from the reference program's by a relative error of at most 0.012.
Values are sent between devices in bfloat16 or wider.
A program may use at most 2 GiB of HBM per device.

```python
import jax
import jax.numpy as jnp

BATCH = 32
CACHE = 4096
HEADS = 64
KV_HEADS = 64
HEAD = 112


def setup_inputs(seed: int = 0, part: int = 0) -> dict:
    kq, kk, kv = (jax.random.fold_in(k, part) for k in jax.random.split(jax.random.key(seed), 3))
    return {
        "q": (3 * jax.random.normal(kq, (BATCH, HEADS, HEAD), jnp.float32)).astype(jnp.bfloat16),
        "k": jax.random.normal(kk, (BATCH, CACHE, KV_HEADS, HEAD), jnp.float32).astype(jnp.bfloat16),
        "v": jax.random.normal(kv, (BATCH, CACHE, KV_HEADS, HEAD), jnp.float32).astype(jnp.bfloat16),
    }


def einsum(form, a, b):
    return jnp.einsum(form, a.astype(jnp.float32), b.astype(jnp.float32))


def reference(q, k, v):
    grouped = q.reshape(BATCH, KV_HEADS, -1, HEAD)
    scores = einsum("bgsd,bugd->bgsu", grouped, k) * HEAD**-0.5
    weights = jax.nn.softmax(scores, -1).astype(jnp.bfloat16)
    return einsum("bgsu,bugd->bgsd", weights, v).astype(jnp.bfloat16).reshape(BATCH, HEADS, HEAD)
```

```python
import functools

import jax
import jax.numpy as jnp
from jax import lax
from jax.experimental import pallas as pl
from jax.experimental.pallas import tpu as pltpu
from jax.sharding import PartitionSpec as P

F32 = jnp.float32
BF16 = jnp.bfloat16
DEPTH = 6
LAG = 5
PIECE = 16
OWNERS = 8


def owner_of(turn, piece):
    inner, upper = turn // 4, turn % 2
    return piece * 8 + (3 * upper + inner * (1 - 2 * upper)) * 2 + (turn % 4) // 2


def place_of(me):
    z = (me // 2) % 4
    return 4 * (((z + 1) // 2) % 2) + 2 * (me % 2) + z // 2, me // 8


def scores(q, keys, scale):
    row = lax.broadcasted_iota(jnp.int32, (8, 1), 0)
    tokens = keys(0).shape[1]
    left = right = jnp.zeros((8, tokens), F32)
    for i in range(8):
        got = jnp.dot(q, jnp.concatenate([keys(i), keys(8 + i)], 1), preferred_element_type=F32)
        left = jnp.where(row == i, got[:8, :tokens], left)
        right = jnp.where(row == i, got[8:, tokens:], right)
    score = jnp.concatenate([left, right], 0) * scale
    high = jnp.max(score, -1, keepdims=True)
    weight = jnp.exp(score - high)
    total = jnp.sum(weight, -1, keepdims=True)
    zero = jnp.zeros((8, tokens), F32)
    left = jnp.concatenate([weight[:8], zero], 1)
    right = jnp.concatenate([zero, weight[8:]], 1)
    return jnp.concatenate([left, right], 0).astype(BF16), total, high


def values(weight, vals):
    row = lax.broadcasted_iota(jnp.int32, (8, 1), 0)
    left = right = jnp.zeros((8, vals(0).shape[0]), F32)
    for i in range(8):
        both = jnp.concatenate([vals(i), vals(8 + i)], 1)
        got = lax.dot_general(weight, both, (((1,), (1,)), ((), ())), preferred_element_type=F32)
        left = jnp.where(row == i, got[:8], left)
        right = jnp.where(row == i, got[8:], right)
    return jnp.concatenate([left, right], 0)


def kernel(n, q_ref, k_hbm, v_hbm, o_ref, kbuf, vbuf, part, full, stat, rpart, rstat, ksem, vsem, psend, ssend, asend, precv, srecv, arecv):
    batch, heads, head = q_ref.shape
    pieces = heads // PIECE
    rounds = batch // OWNERS
    me = lax.axis_index("sp")
    my_turn, my_piece = place_of(me)
    scale = head**-0.5

    def fetch(t, slot):
        k = pltpu.make_async_copy(k_hbm.at[t], kbuf.at[slot], ksem.at[slot])
        v = pltpu.make_async_copy(v_hbm.at[t], vbuf.at[slot], vsem.at[slot])
        return k, v

    def remote(src, dst, send, recv, device):
        return pltpu.make_async_remote_copy(
            src_ref=src, dst_ref=dst, send_sem=send, recv_sem=recv, device_id={"sp": device}, device_id_type=pl.DeviceIdType.MESH
        )

    def drain(ref, sem):
        pltpu.make_async_copy(ref, ref, sem).wait()

    for t in range(DEPTH):
        for copy in fetch(t, t):
            copy.start()

    barrier = pltpu.get_barrier_semaphore()

    def greet(i, _):
        pl.semaphore_signal(barrier, inc=1, device_id={"sp": lax.rem(me + 1 + i, n)}, device_id_type=pl.DeviceIdType.MESH)
        return 0

    lax.fori_loop(0, n - 1, greet, 0)
    pl.semaphore_wait(barrier, n - 1)

    lane = lax.broadcasted_iota(jnp.int32, (PIECE, 128), 1)
    row = lax.broadcasted_iota(jnp.int32, (PIECE, 128), 0)

    def combine(turn):
        t = turn * OWNERS + my_turn
        rows = pl.ds(pl.multiple_of(my_piece * PIECE, PIECE), PIECE)
        drain(rpart.at[pl.ds(turn * n, n - 1)], precv.at[turn])
        drain(rstat.at[pl.ds(turn * n, n - 1)], srecv.at[turn])
        rpart[turn * n + me] = jnp.zeros((PIECE, head), BF16)
        own = stat[t]
        rstat[turn * n + me] = own
        got = rstat[pl.ds(turn * n, n)].reshape(n, 128)
        high = jnp.max(got, 0, keepdims=True)
        weight = jnp.exp(got - high)
        total = jnp.sum(pltpu.roll(got, 64, 1) * weight, 0, keepdims=True)
        share = weight / total
        mask = lane == my_piece * PIECE + row

        def column(line):
            return jnp.sum(jnp.where(mask, line, 0.0), -1, keepdims=True)

        acc = full[t, rows, :] * column(jnp.exp(own - high) / total)
        for src in range(n):
            acc += rpart[turn * n + src].astype(F32) * column(share[src : src + 1])
        o_ref[t, rows, :] = acc.astype(o_ref.dtype)

        def spread(i, _):
            piece = o_ref.at[t, rows]
            remote(piece, piece, asend, arecv, lax.rem(me + 1 + i, n)).start()
            return 0

        lax.fori_loop(0, n - 1, spread, 0)

    def step(t, _):
        slot = lax.rem(t, DEPTH)
        for copy in fetch(t, slot):
            copy.wait()
        got = [scores(q_ref[t, pl.ds(PIECE * c, PIECE), :], lambda i: kbuf[slot, PIECE * c + i], scale) for c in range(pieces)]
        line = jnp.zeros((PIECE, 128), F32)
        for c, (_, total, high) in enumerate(got):
            line = jnp.where(lane == PIECE * c + row, high, line)
            line = jnp.where(lane == heads + PIECE * c + row, total, line)
        stat[t] = jnp.sum(line, 0, keepdims=True)
        for c, (weight, _, _) in enumerate(got):
            out = values(weight, lambda i: vbuf[slot, PIECE * c + i])
            full[t, pl.ds(PIECE * c, PIECE), :] = out
            part[t, pl.ds(PIECE * c, PIECE), :] = out.astype(BF16)

        @pl.when(t + DEPTH < batch)
        def _():
            for copy in fetch(t + DEPTH, slot):
                copy.start()

        turn, place = t // OWNERS, lax.rem(t, OWNERS)
        for c in range(pieces):
            owner = owner_of(place, c)

            @pl.when(owner != me)
            def _():
                remote(part.at[t, pl.ds(PIECE * c, PIECE)], rpart.at[turn * n + me], psend, precv.at[turn], owner).start()
                remote(stat.at[t], rstat.at[turn * n + me], ssend, srecv.at[turn], owner).start()

        late = t - my_turn - LAG

        @pl.when((late >= 0) & (lax.rem(late + OWNERS, OWNERS) == 0))
        def _():
            combine(late // OWNERS)

        return 0

    lax.fori_loop(0, batch, step, 0)

    @pl.when(my_turn + LAG >= OWNERS)
    def _():
        combine(rounds - 1)

    drain(part.at[pl.ds(0, n - 1)], psend)
    drain(rstat.at[pl.ds(0, (n - 1) * rounds)], ssend)
    drain(o_ref.at[pl.ds(0, n - 1)], asend)
    drain(o_ref.at[pl.ds(0, n - 1)], arecv)


def solution(mesh):
    n = mesh.shape["sp"]

    def step(q, k, v):
        batch, tokens, heads, head = k.shape
        rounds, pieces = batch // OWNERS, heads // PIECE
        return pl.pallas_call(
            functools.partial(kernel, n),
            out_shape=jax.ShapeDtypeStruct(q.shape, q.dtype),
            in_specs=[pl.BlockSpec(memory_space=pltpu.VMEM), pl.BlockSpec(memory_space=pl.ANY), pl.BlockSpec(memory_space=pl.ANY)],
            out_specs=pl.BlockSpec(memory_space=pltpu.VMEM),
            scratch_shapes=[
                pltpu.VMEM((DEPTH, heads, head, tokens), k.dtype),
                pltpu.VMEM((DEPTH, heads, head, tokens), v.dtype),
                pltpu.VMEM((batch, heads, head), BF16),
                pltpu.VMEM((batch, heads, head), F32),
                pltpu.VMEM((batch, 1, 128), F32),
                pltpu.VMEM((rounds * n, PIECE, head), BF16),
                pltpu.VMEM((rounds * n, 1, 128), F32),
                pltpu.SemaphoreType.DMA((DEPTH,)),
                pltpu.SemaphoreType.DMA((DEPTH,)),
                pltpu.SemaphoreType.DMA,
                pltpu.SemaphoreType.DMA,
                pltpu.SemaphoreType.DMA,
                pltpu.SemaphoreType.DMA((rounds,)),
                pltpu.SemaphoreType.DMA((rounds,)),
                pltpu.SemaphoreType.DMA,
            ],
            compiler_params=pltpu.CompilerParams(vmem_limit_bytes=60 << 20, collective_id=0, has_side_effects=True),
        )(q, k.transpose(0, 2, 3, 1), v.transpose(0, 2, 3, 1))

    return jax.shard_map(
        step,
        mesh=mesh,
        in_specs=(P("dp", None, None), P("dp", "sp", None, None), P("dp", "sp", None, None)),
        out_specs=P("dp", None, None),
        check_vma=False,
    )
```

```python
import functools

import jax
import jax.numpy as jnp
from jax import lax
from jax.experimental import pallas as pl
from jax.experimental.pallas import tpu as pltpu
from jax.sharding import PartitionSpec as P

F32 = jnp.float32
BF16 = jnp.bfloat16
DEPTH = 5
LAG = 7
PIECE = 16
OWNERS = 8


def flip(z, piece):
    return z + (piece % 2) * (3 - 2 * z)


def owner_of(turn, piece):
    inner, upper = turn // 4, turn % 2
    return piece * 8 + flip(3 * upper + inner * (1 - 2 * upper), piece) * 2 + (turn % 4) // 2


def place_of(me):
    piece = me // 8
    z = flip((me // 2) % 4, piece)
    return 4 * (((z + 1) // 2) % 2) + 2 * (me % 2) + z // 2, piece


def scores(q, keys, scale):
    row = lax.broadcasted_iota(jnp.int32, (8, 1), 0)
    tokens = keys(0).shape[1]
    left = right = jnp.zeros((8, tokens), F32)
    for i in range(8):
        got = jnp.dot(q, jnp.concatenate([keys(i), keys(8 + i)], 1), preferred_element_type=F32)
        left = jnp.where(row == i, got[:8, :tokens], left)
        right = jnp.where(row == i, got[8:, tokens:], right)
    score = jnp.concatenate([left, right], 0) * scale
    high = jnp.max(score, -1, keepdims=True)
    weight = jnp.exp(score - high)
    total = jnp.sum(weight, -1, keepdims=True)
    zero = jnp.zeros((8, tokens), F32)
    left = jnp.concatenate([weight[:8], zero], 1)
    right = jnp.concatenate([zero, weight[8:]], 1)
    return jnp.concatenate([left, right], 0).astype(BF16), total, high


def values(weight, vals):
    row = lax.broadcasted_iota(jnp.int32, (8, 1), 0)
    left = right = jnp.zeros((8, vals(0).shape[0]), F32)
    for i in range(8):
        both = jnp.concatenate([vals(i), vals(8 + i)], 1)
        got = lax.dot_general(weight, both, (((1,), (1,)), ((), ())), preferred_element_type=F32)
        left = jnp.where(row == i, got[:8], left)
        right = jnp.where(row == i, got[8:], right)
    return jnp.concatenate([left, right], 0)


def kernel(n, q_hbm, k_hbm, v_hbm, o_ref, q_ref, kbuf, vbuf, part, full, stat, rpart, rstat, qsem, ksem, vsem, psend, ssend, asend, precv, srecv, arecv):
    batch, heads, head = q_ref.shape
    queries = pltpu.make_async_copy(q_hbm, q_ref, qsem)
    pieces = heads // PIECE
    rounds = batch // OWNERS
    me = lax.axis_index("sp")
    my_turn, my_piece = place_of(me)
    scale = head**-0.5

    def fetch(t, slot):
        k = pltpu.make_async_copy(k_hbm.at[t], kbuf.at[slot], ksem.at[slot])
        v = pltpu.make_async_copy(v_hbm.at[t], vbuf.at[slot], vsem.at[slot])
        return k, v

    def remote(src, dst, send, recv, device):
        return pltpu.make_async_remote_copy(
            src_ref=src, dst_ref=dst, send_sem=send, recv_sem=recv, device_id={"sp": device}, device_id_type=pl.DeviceIdType.MESH
        )

    def drain(ref, sem):
        pltpu.make_async_copy(ref, ref, sem).wait()

    queries.start()
    for t in range(DEPTH):
        for copy in fetch(t, t):
            copy.start()

    barrier = pltpu.get_barrier_semaphore()

    def greet(i, _):
        pl.semaphore_signal(barrier, inc=1, device_id={"sp": lax.rem(me + 1 + i, n)}, device_id_type=pl.DeviceIdType.MESH)
        return 0

    lax.fori_loop(0, n - 1, greet, 0)
    pl.semaphore_wait(barrier, n - 1)
    queries.wait()

    lane = lax.broadcasted_iota(jnp.int32, (PIECE, 128), 1)
    row = lax.broadcasted_iota(jnp.int32, (PIECE, 128), 0)

    def combine(turn):
        t = turn * OWNERS + my_turn
        rows = pl.ds(pl.multiple_of(my_piece * PIECE, PIECE), PIECE)
        drain(rpart.at[pl.ds(turn * n, n - 1)], precv.at[turn])
        drain(rstat.at[pl.ds(turn * n, n - 1)], srecv.at[turn])
        rpart[turn * n + me] = jnp.zeros((PIECE, head), BF16)
        own = stat[t]
        rstat[turn * n + me] = own
        got = rstat[pl.ds(turn * n, n)].reshape(n, 128)
        high = jnp.max(got, 0, keepdims=True)
        weight = jnp.exp(got - high)
        total = jnp.sum(pltpu.roll(got, 64, 1) * weight, 0, keepdims=True)
        share = weight / total
        mask = lane == my_piece * PIECE + row

        def column(line):
            return jnp.sum(jnp.where(mask, line, 0.0), -1, keepdims=True)

        acc = full[t, rows, :] * column(jnp.exp(own - high) / total)
        for src in range(n):
            acc += rpart[turn * n + src].astype(F32) * column(share[src : src + 1])
        o_ref[t, rows, :] = acc.astype(o_ref.dtype)

        def spread(i, _):
            piece = o_ref.at[t, rows]
            remote(piece, piece, asend, arecv, i + (i >= me).astype(jnp.int32)).start()
            return 0

        lax.fori_loop(0, n - 1, spread, 0)

    def post(t):
        turn, place = t // OWNERS, lax.rem(t, OWNERS)

        def send(c):
            rows = pl.ds(pl.multiple_of(PIECE * c, PIECE), PIECE)
            owner = owner_of(place, c)
            remote(part.at[t, rows], rpart.at[turn * n + me], psend, precv.at[turn], owner).start()
            remote(stat.at[t], rstat.at[turn * n + me], ssend, srecv.at[turn], owner).start()

        @pl.when(place != my_turn)
        def _():
            for c in range(pieces):
                send(c)

        @pl.when(place == my_turn)
        def _():
            for c in range(1, pieces):
                send((my_piece + c) % pieces)

    def step(t, _):
        slot = lax.rem(t, DEPTH)
        key, value = fetch(t, slot)
        key.wait()
        value.wait()
        got = [scores(q_ref[t, pl.ds(PIECE * c, PIECE), :], lambda i: kbuf[slot, PIECE * c + i], scale) for c in range(pieces)]
        line = jnp.zeros((PIECE, 128), F32)
        for c, (_, total, high) in enumerate(got):
            line = jnp.where(lane == PIECE * c + row, high, line)
            line = jnp.where(lane == heads + PIECE * c + row, total, line)
        stat[t] = jnp.sum(line, 0, keepdims=True)
        for c, (weight, _, _) in enumerate(got):
            out = values(weight, lambda i: vbuf[slot, PIECE * c + i])
            full[t, pl.ds(PIECE * c, PIECE), :] = out
            part[t, pl.ds(PIECE * c, PIECE), :] = out.astype(BF16)

        @pl.when(t + DEPTH < batch)
        def _():
            for copy in fetch(t + DEPTH, slot):
                copy.start()

        post(t)

        late = t - my_turn - LAG

        @pl.when((late >= 0) & (lax.rem(late + OWNERS, OWNERS) == 0))
        def _():
            combine(late // OWNERS)

        return 0

    lax.fori_loop(0, batch, step, 0)

    @pl.when(my_turn + LAG >= OWNERS)
    def _():
        combine(rounds - 1)

    drain(part.at[pl.ds(0, n - 1)], psend)
    drain(rstat.at[pl.ds(0, (n - 1) * rounds)], ssend)
    drain(o_ref.at[pl.ds(0, n - 1)], asend)
    drain(o_ref.at[pl.ds(0, n - 1)], arecv)


def solution(mesh):
    n = mesh.shape["sp"]

    def step(q, k, v):
        batch, tokens, heads, head = k.shape
        rounds, pieces = batch // OWNERS, heads // PIECE
        return pl.pallas_call(
            functools.partial(kernel, n),
            out_shape=pltpu.VMEM(q.shape, q.dtype),
            in_specs=[pl.BlockSpec(memory_space=pl.ANY)] * 3,
            out_specs=pl.BlockSpec(memory_space=pltpu.VMEM),
            scratch_shapes=[
                pltpu.VMEM(q.shape, q.dtype),
                pltpu.VMEM((DEPTH, heads, head, tokens), k.dtype),
                pltpu.VMEM((DEPTH, heads, head, tokens), v.dtype),
                pltpu.VMEM((batch, heads, head), BF16),
                pltpu.VMEM((batch, heads, head), F32),
                pltpu.VMEM((batch, 1, 128), F32),
                pltpu.VMEM((rounds * n, PIECE, head), BF16),
                pltpu.VMEM((rounds * n, 1, 128), F32),
                pltpu.SemaphoreType.DMA,
                pltpu.SemaphoreType.DMA((DEPTH,)),
                pltpu.SemaphoreType.DMA((DEPTH,)),
                pltpu.SemaphoreType.DMA,
                pltpu.SemaphoreType.DMA,
                pltpu.SemaphoreType.DMA,
                pltpu.SemaphoreType.DMA((rounds,)),
                pltpu.SemaphoreType.DMA((rounds,)),
                pltpu.SemaphoreType.DMA,
            ],
            compiler_params=pltpu.CompilerParams(vmem_limit_bytes=60 << 20, collective_id=0, has_side_effects=True),
        )(q, k.transpose(0, 2, 3, 1), v.transpose(0, 2, 3, 1))

    return jax.shard_map(
        step,
        mesh=mesh,
        in_specs=(P("dp", None, None), P("dp", "sp", None, None), P("dp", "sp", None, None)),
        out_specs=P("dp", None, None),
        check_vma=False,
    )
```

```python
import functools

import jax
import jax.numpy as jnp
from jax import lax
from jax.experimental import pallas as pl
from jax.experimental.pallas import tpu as pltpu
from jax.sharding import PartitionSpec as P

F32 = jnp.float32
BF16 = jnp.bfloat16
DEPTH = 5
LAG = 7
PIECE = 16
OWNERS = 8


def flip(z, piece):
    return z + (piece % 2) * (3 - 2 * z)


def owner_of(turn, piece):
    inner, upper = turn // 4, turn % 2
    return piece * 8 + flip(3 * upper + inner * (1 - 2 * upper), piece) * 2 + (turn % 4) // 2


def place_of(me):
    piece = me // 8
    z = flip((me // 2) % 4, piece)
    return 4 * (((z + 1) // 2) % 2) + 2 * (me % 2) + z // 2, piece


def scores(q, keys, scale):
    row = lax.broadcasted_iota(jnp.int32, (8, 1), 0)
    tokens = keys(0).shape[1]
    left = right = jnp.zeros((8, tokens), F32)
    for i in range(8):
        got = jnp.dot(q, jnp.concatenate([keys(i), keys(8 + i)], 1), preferred_element_type=F32)
        left = jnp.where(row == i, got[:8, :tokens], left)
        right = jnp.where(row == i, got[8:, tokens:], right)
    score = jnp.concatenate([left, right], 0) * scale
    high = jnp.max(score, -1, keepdims=True)
    weight = jnp.exp(score - high)
    total = jnp.sum(weight, -1, keepdims=True)
    zero = jnp.zeros((8, tokens), F32)
    left = jnp.concatenate([weight[:8], zero], 1)
    right = jnp.concatenate([zero, weight[8:]], 1)
    return jnp.concatenate([left, right], 0).astype(BF16), total, high


def values(first, second, vals):
    row = lax.broadcasted_iota(jnp.int32, (8, 1), 0)
    lane = lax.broadcasted_iota(jnp.int32, (1, 16), 1) % 8
    head = vals(0).shape[0]
    left = right = jnp.zeros((8, head), F32)
    turned = jnp.zeros((head, 16), F32)
    contract = (((1,), (1,)), ((), ()))
    for i in range(0, 8, 2):
        for j in (i, i + 1):
            both = jnp.concatenate([vals(j), vals(8 + j)], 1)
            got = lax.dot_general(first, both, contract, preferred_element_type=F32)
            left = jnp.where(row == j, got[:8], left)
            right = jnp.where(row == j, got[8:], right)
        for j in (i, i + 1):
            both = jnp.concatenate([vals(16 + j), vals(24 + j)], 1)
            got = lax.dot_general(both, second, contract, preferred_element_type=F32)
            turned = jnp.where(lane == j, got, turned)
    return jnp.concatenate([left, right], 0), turned.T


def kernel(n, q_hbm, k_hbm, v_hbm, o_ref, q_ref, kbuf, vbuf, part, full, stat, rpart, rstat, qsem, ksem, vsem, psend, ssend, asend, precv, srecv, arecv):
    batch, heads, head = q_ref.shape
    queries = pltpu.make_async_copy(q_hbm, q_ref, qsem)
    pieces = heads // PIECE
    rounds = batch // OWNERS
    me = lax.axis_index("sp")
    my_turn, my_piece = place_of(me)
    scale = head**-0.5

    def fetch(t, slot):
        k = pltpu.make_async_copy(k_hbm.at[t], kbuf.at[slot], ksem.at[slot])
        v = pltpu.make_async_copy(v_hbm.at[t], vbuf.at[slot], vsem.at[slot])
        return k, v

    def remote(src, dst, send, recv, device):
        return pltpu.make_async_remote_copy(
            src_ref=src, dst_ref=dst, send_sem=send, recv_sem=recv, device_id={"sp": device}, device_id_type=pl.DeviceIdType.MESH
        )

    def drain(ref, sem):
        pltpu.make_async_copy(ref, ref, sem).wait()

    queries.start()
    for t in range(DEPTH):
        for copy in fetch(t, t):
            copy.start()

    barrier = pltpu.get_barrier_semaphore()

    def greet(i, _):
        pl.semaphore_signal(barrier, inc=1, device_id={"sp": lax.rem(me + 1 + i, n)}, device_id_type=pl.DeviceIdType.MESH)
        return 0

    lax.fori_loop(0, n - 1, greet, 0)
    pl.semaphore_wait(barrier, n - 1)
    queries.wait()

    lane = lax.broadcasted_iota(jnp.int32, (PIECE, 128), 1)
    row = lax.broadcasted_iota(jnp.int32, (PIECE, 128), 0)

    def combine(turn):
        t = turn * OWNERS + my_turn
        rows = pl.ds(pl.multiple_of(my_piece * PIECE, PIECE), PIECE)
        drain(rpart.at[pl.ds(turn * n, n - 1)], precv.at[turn])
        drain(rstat.at[pl.ds(turn * n, n - 1)], srecv.at[turn])
        rpart[turn * n + me] = jnp.zeros((PIECE, head), BF16)
        own = stat[t]
        rstat[turn * n + me] = own
        got = rstat[pl.ds(turn * n, n)].reshape(n, 128)
        high = jnp.max(got, 0, keepdims=True)
        weight = jnp.exp(got - high)
        total = jnp.sum(pltpu.roll(got, 64, 1) * weight, 0, keepdims=True)
        share = weight / total
        mask = lane == my_piece * PIECE + row

        def column(line):
            return jnp.sum(jnp.where(mask, line, 0.0), -1, keepdims=True)

        acc = full[t, rows, :] * column(jnp.exp(own - high) / total)
        for src in range(n):
            acc += rpart[turn * n + src].astype(F32) * column(share[src : src + 1])
        o_ref[t, rows, :] = acc.astype(o_ref.dtype)

        def spread(i, _):
            piece = o_ref.at[t, rows]
            there = jnp.where(t == batch - 1, i + (i >= me).astype(jnp.int32), lax.rem(me + 1 + i, n))
            remote(piece, piece, asend, arecv, there).start()
            return 0

        lax.fori_loop(0, n - 1, spread, 0)

    def post(t):
        turn, place = t // OWNERS, lax.rem(t, OWNERS)

        def send(c):
            rows = pl.ds(pl.multiple_of(PIECE * c, PIECE), PIECE)
            owner = owner_of(place, c)
            remote(part.at[t, rows], rpart.at[turn * n + me], psend, precv.at[turn], owner).start()
            remote(stat.at[t], rstat.at[turn * n + me], ssend, srecv.at[turn], owner).start()

        @pl.when(place != my_turn)
        def _():
            for c in range(pieces - 1, -1, -1):
                send(c)

        @pl.when(place == my_turn)
        def _():
            for c in range(1, pieces):
                send((my_piece + c) % pieces)

    def step(t, _):
        slot = lax.rem(t, DEPTH)
        key, value = fetch(t, slot)
        key.wait()
        value.wait()
        got = [scores(q_ref[t, pl.ds(PIECE * c, PIECE), :], lambda i: kbuf[slot, PIECE * c + i], scale) for c in range(pieces)]
        line = jnp.zeros((PIECE, 128), F32)
        for c, (_, total, high) in enumerate(got):
            line = jnp.where(lane == PIECE * c + row, high, line)
            line = jnp.where(lane == heads + PIECE * c + row, total, line)
        stat[t] = jnp.sum(line, 0, keepdims=True)
        for c in range(0, pieces, 2):
            outs = values(got[c][0], got[c + 1][0], lambda i: vbuf[slot, PIECE * c + i])
            for d, out in enumerate(outs):
                rows = pl.ds(PIECE * (c + d), PIECE)
                full[t, rows, :] = out
                part[t, rows, :] = out.astype(BF16)

        @pl.when(t + DEPTH < batch)
        def _():
            for copy in fetch(t + DEPTH, slot):
                copy.start()

        post(t)

        late = t - my_turn - LAG

        @pl.when((late >= 0) & (lax.rem(late + OWNERS, OWNERS) == 0))
        def _():
            combine(late // OWNERS)

        return 0

    lax.fori_loop(0, batch, step, 0)

    @pl.when(my_turn + LAG >= OWNERS)
    def _():
        combine(rounds - 1)

    drain(part.at[pl.ds(0, n - 1)], psend)
    drain(rstat.at[pl.ds(0, (n - 1) * rounds)], ssend)
    drain(o_ref.at[pl.ds(0, n - 1)], asend)
    drain(o_ref.at[pl.ds(0, n - 1)], arecv)


def solution(mesh):
    n = mesh.shape["sp"]

    def step(q, k, v):
        batch, tokens, heads, head = k.shape
        rounds, pieces = batch // OWNERS, heads // PIECE
        return pl.pallas_call(
            functools.partial(kernel, n),
            out_shape=pltpu.VMEM(q.shape, q.dtype),
            in_specs=[pl.BlockSpec(memory_space=pl.ANY)] * 3,
            out_specs=pl.BlockSpec(memory_space=pltpu.VMEM),
            scratch_shapes=[
                pltpu.VMEM(q.shape, q.dtype),
                pltpu.VMEM((DEPTH, heads, head, tokens), k.dtype),
                pltpu.VMEM((DEPTH, heads, head, tokens), v.dtype),
                pltpu.VMEM((batch, heads, head), BF16),
                pltpu.VMEM((batch, heads, head), F32),
                pltpu.VMEM((batch, 1, 128), F32),
                pltpu.VMEM((rounds * n, PIECE, head), BF16),
                pltpu.VMEM((rounds * n, 1, 128), F32),
                pltpu.SemaphoreType.DMA,
                pltpu.SemaphoreType.DMA((DEPTH,)),
                pltpu.SemaphoreType.DMA((DEPTH,)),
                pltpu.SemaphoreType.DMA,
                pltpu.SemaphoreType.DMA,
                pltpu.SemaphoreType.DMA,
                pltpu.SemaphoreType.DMA((rounds,)),
                pltpu.SemaphoreType.DMA((rounds,)),
                pltpu.SemaphoreType.DMA,
            ],
            compiler_params=pltpu.CompilerParams(vmem_limit_bytes=60 << 20, collective_id=0, has_side_effects=True),
        )(q, k.transpose(0, 2, 3, 1), v.transpose(0, 2, 3, 1))

    return jax.shard_map(
        step,
        mesh=mesh,
        in_specs=(P("dp", None, None), P("dp", "sp", None, None), P("dp", "sp", None, None)),
        out_specs=P("dp", None, None),
        check_vma=False,
    )
```

```python
import functools

import jax
import jax.numpy as jnp
from jax import lax
from jax.experimental import pallas as pl
from jax.experimental.pallas import tpu as pltpu
from jax.sharding import PartitionSpec as P

F32 = jnp.float32
BF16 = jnp.bfloat16
DEPTH = 5
LAG = 7
PIECE = 16
OWNERS = 8


def flip(z, piece):
    return z + (piece % 2) * (3 - 2 * z)


def owner_of(turn, piece):
    inner, upper = turn // 4, turn % 2
    return piece * 8 + flip(3 * upper + inner * (1 - 2 * upper), piece) * 2 + (turn % 4) // 2


def place_of(me):
    piece = me // 8
    z = flip((me // 2) % 4, piece)
    return 4 * (((z + 1) // 2) % 2) + 2 * (me % 2) + z // 2, piece


def scores(q, keys, scale):
    row = lax.broadcasted_iota(jnp.int32, (8, 1), 0)
    tokens = keys(0).shape[1]
    left = right = jnp.zeros((8, tokens), F32)
    for i in range(8):
        got = jnp.dot(q, jnp.concatenate([keys(i), keys(8 + i)], 1), preferred_element_type=F32)
        left = jnp.where(row == i, got[:8, :tokens], left)
        right = jnp.where(row == i, got[8:, tokens:], right)
    score = jnp.concatenate([left, right], 0) * scale
    high = jnp.max(score, -1, keepdims=True)
    weight = jnp.exp(score - high)
    total = jnp.sum(weight, -1, keepdims=True)
    zero = jnp.zeros((8, tokens), F32)
    left = jnp.concatenate([weight[:8], zero], 1)
    right = jnp.concatenate([zero, weight[8:]], 1)
    return jnp.concatenate([left, right], 0).astype(BF16), total, high


def values(first, second, vals):
    row = lax.broadcasted_iota(jnp.int32, (8, 1), 0)
    lane = lax.broadcasted_iota(jnp.int32, (1, 16), 1) % 8
    head = vals(0).shape[0]
    left = right = jnp.zeros((8, head), F32)
    turned = jnp.zeros((head, 16), F32)
    contract = (((1,), (1,)), ((), ()))
    for i in range(0, 8, 2):
        for j in (i, i + 1):
            both = jnp.concatenate([vals(j), vals(8 + j)], 1)
            got = lax.dot_general(first, both, contract, preferred_element_type=F32)
            left = jnp.where(row == j, got[:8], left)
            right = jnp.where(row == j, got[8:], right)
        for j in (i, i + 1):
            both = jnp.concatenate([vals(16 + j), vals(24 + j)], 1)
            got = lax.dot_general(both, second, contract, preferred_element_type=F32)
            turned = jnp.where(lane == j, got, turned)
    return jnp.concatenate([left, right], 0), turned.T


def kernel(n, q_hbm, k_hbm, v_hbm, o_ref, q_ref, kbuf, vbuf, part, full, stat, rpart, rstat, qsem, ksem, vsem, psend, ssend, asend, precv, srecv, arecv):
    batch, heads, head = q_ref.shape
    queries = pltpu.make_async_copy(q_hbm, q_ref, qsem)
    pieces = heads // PIECE
    rounds = batch // OWNERS
    me = lax.axis_index("sp")
    my_turn, my_piece = place_of(me)
    scale = head**-0.5

    def fetch(t, slot):
        k = pltpu.make_async_copy(k_hbm.at[t], kbuf.at[slot], ksem.at[slot])
        v = pltpu.make_async_copy(v_hbm.at[t], vbuf.at[slot], vsem.at[slot])
        return k, v

    def remote(src, dst, send, recv, device):
        return pltpu.make_async_remote_copy(
            src_ref=src, dst_ref=dst, send_sem=send, recv_sem=recv, device_id={"sp": device}, device_id_type=pl.DeviceIdType.MESH
        )

    def drain(ref, sem):
        pltpu.make_async_copy(ref, ref, sem).wait()

    queries.start()
    for t in range(DEPTH):
        for copy in fetch(t, t):
            copy.start()

    barrier = pltpu.get_barrier_semaphore()

    def greet(i, _):
        pl.semaphore_signal(barrier, inc=1, device_id={"sp": lax.rem(me + 1 + i, n)}, device_id_type=pl.DeviceIdType.MESH)
        return 0

    lax.fori_loop(0, n - 1, greet, 0)
    pl.semaphore_wait(barrier, n - 1)
    queries.wait()

    lane = lax.broadcasted_iota(jnp.int32, (PIECE, 128), 1)
    row = lax.broadcasted_iota(jnp.int32, (PIECE, 128), 0)

    def combine(turn):
        t = turn * OWNERS + my_turn
        rows = pl.ds(pl.multiple_of(my_piece * PIECE, PIECE), PIECE)
        drain(rpart.at[pl.ds(turn * n, n - 1)], precv.at[turn])
        drain(rstat.at[pl.ds(turn * n, n - 1)], srecv.at[turn])
        rpart[turn * n + me] = jnp.zeros((PIECE, head), BF16)
        own = stat[t]
        rstat[turn * n + me] = own
        got = rstat[pl.ds(turn * n, n)].reshape(n, 128)
        high = jnp.max(got, 0, keepdims=True)
        weight = jnp.exp(got - high)
        total = jnp.sum(pltpu.roll(got, 64, 1) * weight, 0, keepdims=True)
        share = weight / total
        mask = lane == my_piece * PIECE + row

        def column(line):
            return jnp.sum(jnp.where(mask, line, 0.0), -1, keepdims=True)

        acc = full[t, rows, :] * column(jnp.exp(own - high) / total)
        sums = [acc, *[jnp.zeros((PIECE, head), F32)] * 3]
        for src in range(n):
            sums[src % 4] += rpart[turn * n + src].astype(F32) * column(share[src : src + 1])
        o_ref[t, rows, :] = ((sums[0] + sums[1]) + (sums[2] + sums[3])).astype(o_ref.dtype)

        def spread(i, _):
            piece = o_ref.at[t, rows]
            there = jnp.where(t == batch - 1, i + (i >= me).astype(jnp.int32), lax.rem(me + 1 + i, n))
            remote(piece, piece, asend, arecv, there).start()
            return 0

        lax.fori_loop(0, n - 1, spread, 0)

    def post(t):
        turn, place = t // OWNERS, lax.rem(t, OWNERS)

        def send(c):
            rows = pl.ds(pl.multiple_of(PIECE * c, PIECE), PIECE)
            owner = owner_of(place, c)
            remote(part.at[t, rows], rpart.at[turn * n + me], psend, precv.at[turn], owner).start()
            remote(stat.at[t], rstat.at[turn * n + me], ssend, srecv.at[turn], owner).start()

        @pl.when(place != my_turn)
        def _():
            for c in range(pieces - 1, -1, -1):
                send(c)

        @pl.when(place == my_turn)
        def _():
            for c in range(1, pieces):
                send((my_piece + c) % pieces)

    def step(t, _):
        slot = lax.rem(t, DEPTH)
        key, value = fetch(t, slot)
        key.wait()
        value.wait()
        got = [scores(q_ref[t, pl.ds(PIECE * c, PIECE), :], lambda i: kbuf[slot, PIECE * c + i], scale) for c in range(pieces)]
        line = jnp.zeros((PIECE, 128), F32)
        for c, (_, total, high) in enumerate(got):
            line = jnp.where(lane == PIECE * c + row, high, line)
            line = jnp.where(lane == heads + PIECE * c + row, total, line)
        stat[t] = jnp.sum(line, 0, keepdims=True)
        for c in range(0, pieces, 2):
            outs = values(got[c][0], got[c + 1][0], lambda i: vbuf[slot, PIECE * c + i])
            for d, out in enumerate(outs):
                rows = pl.ds(PIECE * (c + d), PIECE)
                full[t, rows, :] = out
                part[t, rows, :] = out.astype(BF16)

        @pl.when(t + DEPTH < batch)
        def _():
            for copy in fetch(t + DEPTH, slot):
                copy.start()

        post(t)

        late = t - my_turn - LAG

        @pl.when((late >= 0) & (lax.rem(late + OWNERS, OWNERS) == 0))
        def _():
            combine(late // OWNERS)

        return 0

    lax.fori_loop(0, batch, step, 0)

    @pl.when(my_turn + LAG >= OWNERS)
    def _():
        combine(rounds - 1)

    drain(part.at[pl.ds(0, n - 1)], psend)
    drain(rstat.at[pl.ds(0, (n - 1) * rounds)], ssend)
    drain(o_ref.at[pl.ds(0, n - 1)], asend)
    drain(o_ref.at[pl.ds(0, n - 1)], arecv)


def solution(mesh):
    n = mesh.shape["sp"]

    def step(q, k, v):
        batch, tokens, heads, head = k.shape
        rounds, pieces = batch // OWNERS, heads // PIECE
        return pl.pallas_call(
            functools.partial(kernel, n),
            out_shape=pltpu.VMEM(q.shape, q.dtype),
            in_specs=[pl.BlockSpec(memory_space=pl.ANY)] * 3,
            out_specs=pl.BlockSpec(memory_space=pltpu.VMEM),
            scratch_shapes=[
                pltpu.VMEM(q.shape, q.dtype),
                pltpu.VMEM((DEPTH, heads, head, tokens), k.dtype),
                pltpu.VMEM((DEPTH, heads, head, tokens), v.dtype),
                pltpu.VMEM((batch, heads, head), BF16),
                pltpu.VMEM((batch, heads, head), F32),
                pltpu.VMEM((batch, 1, 128), F32),
                pltpu.VMEM((rounds * n, PIECE, head), BF16),
                pltpu.VMEM((rounds * n, 1, 128), F32),
                pltpu.SemaphoreType.DMA,
                pltpu.SemaphoreType.DMA((DEPTH,)),
                pltpu.SemaphoreType.DMA((DEPTH,)),
                pltpu.SemaphoreType.DMA,
                pltpu.SemaphoreType.DMA,
                pltpu.SemaphoreType.DMA,
                pltpu.SemaphoreType.DMA((rounds,)),
                pltpu.SemaphoreType.DMA((rounds,)),
                pltpu.SemaphoreType.DMA,
            ],
            compiler_params=pltpu.CompilerParams(vmem_limit_bytes=60 << 20, collective_id=0, has_side_effects=True),
        )(q, k.transpose(0, 2, 3, 1), v.transpose(0, 2, 3, 1))

    return jax.shard_map(
        step,
        mesh=mesh,
        in_specs=(P("dp", None, None), P("dp", "sp", None, None), P("dp", "sp", None, None)),
        out_specs=P("dp", None, None),
        check_vma=False,
    )
```
